8 devices in a mesh: cz: 2 (over z, y), cy: 2 (over x), cx: 2 (over core).
Axes of the slice: x: 2, y: 2, z: 1, core: 2. Of those that a mesh axis runs over, the one named last changes fastest.
Arguments:
- x: bfloat16 [512, 2048], P(('cx', 'cz'), 'cy')
- w1: bfloat16 [2048, 8192], P('cy', ('cz', 'cx'))
- w2: bfloat16 [8192, 2048], P('cz', ('cy', 'cx'))
Outputs:
- output: bfloat16 [512, 2048], P(('cx', 'cz'), 'cy')
All inputs are finite; a program needn't handle non-finite values.
Results may differ from the reference program's by a relative error of at most 0.0114559.
Values are sent between devices in bfloat16 or wider.
A program may use at most 1 GiB of HBM per device.

```python
import jax
import jax.numpy as jnp

N = 512
D = 2048
F = 8192


def setup_inputs(seed: int = 0) -> dict:
    k1, k2, k3 = jax.random.split(jax.random.PRNGKey(seed), 3)
    x = jax.random.normal(k1, (N, D), jnp.float32)
    w1 = jax.random.normal(k2, (D, F), jnp.float32) * D ** -0.5
    w2 = jax.random.normal(k3, (F, D), jnp.float32) * F ** -0.5
    return {"x": x.astype(jnp.bfloat16), "w1": w1.astype(jnp.bfloat16), "w2": w2.astype(jnp.bfloat16)}


def reference(x, w1, w2):
    c = jnp.dot(x, w1, preferred_element_type=jnp.float32).astype(jnp.bfloat16)
    h = jax.nn.gelu(c.astype(jnp.float32), approximate=True).astype(jnp.bfloat16)
    return jnp.dot(h, w2, preferred_element_type=jnp.float32).astype(jnp.bfloat16)
```

```python
import functools

import jax
import jax.numpy as jnp
from jax import lax
from jax.experimental import pallas as pl
from jax.experimental.pallas import tpu as pltpu
from jax.sharding import PartitionSpec as P

MESH = pl.DeviceIdType.MESH
F32 = jnp.float32
BF16 = jnp.bfloat16
G = 64


def gelu(c):
    c = c.astype(F32)
    return 0.5 * c * (1.0 + jnp.tanh(0.7978845608028654 * (c + 0.044715 * (c * c * c))))


def kernel(x_ref, w1_ref, w2_ref, out_ref,
           xs, w1s, w1o, w2s, psend, precv, pown, h, zp, zr,
           lsem, xss, xrs, pss, prs, hss, hrs, dss, drs, fss, frs, zss, zrs):
    cz, cy, cx = (lax.axis_index(a) for a in ("cz", "cy", "cx"))
    oz, oy, ox = 1 - cz, 1 - cy, 1 - cx
    dev_x = (cz, oy, cx)
    dev_c = (cz, cy, ox)
    dev_y = (oz, cy, cx)
    dev_d = (oz, cy, ox)

    rows, depth = x_ref.shape
    q = rows // G
    n = 4 * q
    half = w1_ref.shape[1] // 2
    wide = w2_ref.shape[1]

    def own_pair(i):
        return i if i < q // 2 else i + q

    def rcopy(src, dst, ss, rs, dev):
        return pltpu.make_async_remote_copy(src_ref=src, dst_ref=dst, send_sem=ss, recv_sem=rs, device_id=dev,
                                            device_id_type=MESH)

    loads_x = [pltpu.make_async_copy(x_ref.at[pl.ds(i * G, G)], xs.at[2 * own_pair(i)], lsem.at[i]) for i in range(q)]
    load_s = pltpu.make_async_copy(w1_ref.at[:, pl.ds(pl.multiple_of(oy * half, half), half)], w1s, lsem.at[q])
    load_o = pltpu.make_async_copy(w1_ref.at[:, pl.ds(pl.multiple_of(cy * half, half), half)], w1o, lsem.at[q + 1])
    loads_2 = []
    for j, (a, b) in enumerate(((cx, cy), (cx, oy), (ox, cy), (ox, oy))):
        loads_2.append(pltpu.make_async_copy(w2_ref.at[pl.ds(pl.multiple_of((2 * a + b) * half, half), half)], w2s.at[j],
                                             lsem.at[q + 2 + j]))
    for c in loads_x + [load_s, load_o] + loads_2:
        c.start()

    barrier = pltpu.get_barrier_semaphore()
    for dev in (dev_x, dev_c, dev_y, dev_d):
        pl.semaphore_signal(barrier, inc=1, device_id=dev, device_id_type=MESH)
    for c in loads_x:
        c.wait()
    pl.semaphore_wait(barrier, 4)

    x_sends = []
    for i in range(q):
        src = xs.at[2 * own_pair(i)]
        for d, (dev, u) in enumerate(((dev_c, 2 * own_pair(i) + 1), (dev_y, 2 * (i + q // 2)), (dev_d, 2 * (i + q // 2) + 1))):
            c = rcopy(src, xs.at[u], xss.at[d, i], xrs.at[u], dev)
            c.start()
            x_sends.append(c)
    load_s.wait()

    def p_copy(u):
        return rcopy(psend.at[u], precv.at[u], pss.at[u], prs.at[u], dev_x)

    def h_copy(u):
        return rcopy(h.at[0, u], h.at[1, u], hss.at[u], hrs.at[u], dev_x)

    def d_copy(u):
        return rcopy(h.at[0, u], h.at[2, u + 1 - 2 * lax.rem(u, 2)], dss.at[u], drs.at[u + 1 - 2 * lax.rem(u, 2)], dev_c)

    def d_wait(u):
        rcopy(h.at[0, u], h.at[2, u], dss.at[u], drs.at[u], dev_c).wait_recv()

    def f_copy(u):
        return rcopy(h.at[1, u], h.at[3, u + 1 - 2 * lax.rem(u, 2)], fss.at[u], frs.at[u + 1 - 2 * lax.rem(u, 2)], dev_c)

    def f_wait(u):
        rcopy(h.at[1, u], h.at[3, u], fss.at[u], frs.at[u], dev_c).wait_recv()

    def partial(u):
        psend[u] = jnp.dot(xs[u], w1s[...], preferred_element_type=F32)
        p_copy(u).start()

    def stay(u):
        pown[u] = jnp.dot(xs[u], w1o[...], preferred_element_type=F32)

    def x_wait(u):
        rcopy(xs.at[u], xs.at[u], xss.at[0, 0], xrs.at[u], dev_c).wait_recv()

    partial(0)
    load_o.wait()
    stay(0)

    def layer1(u, carry):
        i = lax.rem(u, 2)
        mine = jnp.logical_and(i == 0, jnp.logical_or(u < q, u >= 3 * q))

        @pl.when(jnp.logical_not(mine))
        def _():
            x_wait(u)

        partial(u)
        stay(u)
        return carry

    lax.fori_loop(1, n, layer1, 0)

    def activate(u, carry):
        p_copy(u).wait_recv()
        c = (pown[u] + precv[u]).astype(BF16)
        h[0, u] = gelu(c).astype(BF16)
        h_copy(u).start()
        d_copy(u).start()
        return carry

    lax.fori_loop(0, n, activate, 0)
    for c in loads_2:
        c.wait()

    def forward(u):
        h_copy(u).wait_recv()
        f_copy(u).start()

    def z_dev(u):
        i, k = lax.rem(u, 2), u // 2
        other = jnp.logical_and(k >= q // 2, k < q // 2 + q).astype(jnp.int32)
        late = (k >= q // 2 + q).astype(jnp.int32)
        sub = k - other * (q // 2) - late * q
        dev = (cz + other - 2 * other * cz, cy, cx + i - 2 * i * cx)
        slot = other * (1 + i)
        return dev, slot, sub

    def z_copy(u):
        dev, slot, sub = z_dev(u)
        return rcopy(zp.at[u], zr.at[slot, sub], zss.at[u], zrs.at[slot, sub], dev)

    def kept(u):
        return jnp.logical_and(lax.rem(u, 2) == 0, jnp.logical_or(u < q, u >= 3 * q))

    def second(u):
        acc = jnp.dot(h[0, u], w2s[0], preferred_element_type=F32)
        d_wait(u)
        acc += jnp.dot(h[2, u], w2s[2], preferred_element_type=F32)
        acc += jnp.dot(h[1, u], w2s[1], preferred_element_type=F32)
        f_wait(u)
        acc += jnp.dot(h[3, u], w2s[3], preferred_element_type=F32)
        zp[u] = acc

        @pl.when(jnp.logical_not(kept(u)))
        def _():
            z_copy(u).start()

    forward(0)
    forward(1)

    def layer2(u, carry):
        forward(u + 2)
        second(u)
        return carry

    lax.fori_loop(0, n - 2, layer2, 0)
    second(jnp.int32(n - 2))
    second(jnp.int32(n - 1))

    left = pl.multiple_of(cx * wide, wide)
    right = pl.multiple_of(ox * wide, wide)
    for i in range(q):
        for slot in range(3):
            rcopy(zp.at[0], zr.at[slot, i], zss.at[0], zrs.at[slot, i], dev_c).wait_recv()
        out_ref[pl.ds(i * G, G), pl.ds(left, wide)] = (zp[2 * own_pair(i)] + zr[1, i]).astype(BF16)
        out_ref[pl.ds(i * G, G), pl.ds(right, wide)] = (zr[0, i] + zr[2, i]).astype(BF16)

    for c in x_sends:
        c.wait_send()

    def finish(u, carry):
        p_copy(u).wait_send()
        h_copy(u).wait_send()
        d_copy(u).wait_send()
        f_copy(u).wait_send()

        @pl.when(jnp.logical_not(kept(u)))
        def _():
            z_copy(u).wait_send()

        return carry

    lax.fori_loop(0, n, finish, 0)


def solution(mesh):
    def body(x, w1, w2):
        rows, depth = x.shape
        q = rows // G
        n = 4 * q
        half = w1.shape[1] // 2
        wide = w2.shape[1]
        dma = pltpu.SemaphoreType.DMA
        anywhere = pl.BlockSpec(memory_space=pl.ANY)
        return pl.pallas_call(
            kernel,
            out_shape=jax.ShapeDtypeStruct((rows, 2 * wide), BF16),
            in_specs=[anywhere] * 3,
            out_specs=pl.BlockSpec(memory_space=pltpu.VMEM),
            scratch_shapes=[
                pltpu.VMEM((n, G, depth), BF16),
                pltpu.VMEM((depth, half), BF16),
                pltpu.VMEM((depth, half), BF16),
                pltpu.VMEM((4, half, wide), BF16),
                pltpu.VMEM((n, G, half), F32),
                pltpu.VMEM((n, G, half), F32),
                pltpu.VMEM((n, G, half), F32),
                pltpu.VMEM((4, n, G, half), BF16),
                pltpu.VMEM((n, G, wide), F32),
                pltpu.VMEM((3, q, G, wide), F32),
                dma((q + 6,)),
                dma((3, q)), dma((n,)),
                dma((n,)), dma((n,)),
                dma((n,)), dma((n,)),
                dma((n,)), dma((n,)),
                dma((n,)), dma((n,)),
                dma((n,)), dma((3, q)),
            ],
            compiler_params=pltpu.CompilerParams(
                collective_id=0, has_side_effects=True, vmem_limit_bytes=60 * 1024 * 1024,
            ),
            cost_estimate=pl.CostEstimate(flops=4 * 512 * 1024 * 2048 * 2, bytes_accessed=9 << 20, transcendentals=512 * 1024),
        )(x, w1, w2)

    return jax.shard_map(
        body,
        mesh=mesh,
        in_specs=(P(("cx", "cz"), "cy"), P("cy", ("cz", "cx")), P("cz", ("cy", "cx"))),
        out_specs=P(("cx", "cz"), "cy"),
        check_vma=False,
    )
```

```python
import functools

import jax
import jax.numpy as jnp
from jax import lax
from jax.experimental import pallas as pl
from jax.experimental.pallas import tpu as pltpu
from jax.sharding import PartitionSpec as P

MESH = pl.DeviceIdType.MESH
F32 = jnp.float32
BF16 = jnp.bfloat16
G = 64
LAG = 1
PIECES = 4


def gelu(c):
    c = c.astype(F32)
    return 0.5 * c * (1.0 + jnp.tanh(0.7978845608028654 * (c + 0.044715 * (c * c * c))))


def dot(a, b):
    return jnp.dot(a, b, preferred_element_type=F32)


def kernel(x_ref, w1_ref, w2_ref, out_ref,
           xs, w1s, w1o, w2s, psend, precv, pown, h, zp, zr,
           lsem, xss, xrs, wss, wrs, pss, prs, hss, hrs, zss, zrs):
    cz, cy, cx = (lax.axis_index(a) for a in ("cz", "cy", "cx"))
    oz, oy, ox = 1 - cz, 1 - cy, 1 - cx
    dev_x = (cz, oy, cx)
    dev_c = (cz, cy, ox)
    dev_y = (oz, cy, cx)
    dev_d = (oz, cy, ox)

    rows = x_ref.shape[0]
    q = rows // G
    n = 4 * q
    e = q // 2
    half = w1_ref.shape[1] // 2
    wide = w2_ref.shape[1]
    piece = half // PIECES

    def own_unit(i):
        return 2 * i if i < e else 2 * (i + q) + 1

    def partner_unit(i):
        return 2 * i + 1 if i < e else 2 * (i + q)

    def rcopy(src, dst, ss, rs, dev):
        return pltpu.make_async_remote_copy(src_ref=src, dst_ref=dst, send_sem=ss, recv_sem=rs, device_id=dev,
                                            device_id_type=MESH)

    def block(i, size):
        return pl.ds(pl.multiple_of(i * size, size), size)

    loads_x = [pltpu.make_async_copy(x_ref.at[pl.ds(i * G, G)], xs.at[own_unit(i)], lsem.at[i]) for i in range(q)]
    loads_s = [pltpu.make_async_copy(w1_ref.at[:, pl.ds(pl.multiple_of(oy * half + i * piece, piece), piece)],
                                     w1s.at[:, pl.ds(i * piece, piece)], lsem.at[q + i]) for i in range(PIECES)]
    load_o = pltpu.make_async_copy(w1_ref.at[:, block(cy, half)], w1o, lsem.at[q + PIECES])
    loads_2 = [pltpu.make_async_copy(w2_ref.at[block(2 * cx + b, half)], w2s.at[j, :, block(cx, wide)],
                                     lsem.at[q + PIECES + 1 + j]) for j, b in enumerate((cy, oy))]
    sends_2 = [rcopy(w2_ref.at[block(2 * ox + b, half)], w2s.at[j, :, block(cx, wide)], wss.at[j], wrs.at[j], dev_c)
               for j, b in enumerate((cy, oy))]
    for c in loads_x[:1] + loads_s[:1] + loads_x[1:] + loads_s[1:]:
        c.start()

    barrier = pltpu.get_barrier_semaphore()
    for dev in (dev_x, dev_c, dev_y, dev_d):
        pl.semaphore_signal(barrier, inc=1, device_id=dev, device_id_type=MESH)

    def first(i):
        cols = pl.ds(i * piece, piece)
        loads_s[i].wait()
        psend[0, :, cols] = dot(xs[0], w1s[:, cols])

    def first_send(i):
        cols = pl.ds(i * piece, piece)
        rcopy(psend.at[0, :, cols], precv.at[0, :, cols], pss.at[0], prs.at[0], dev_x).start()

    loads_x[0].wait()
    first(0)
    pl.semaphore_wait(barrier, 4)
    first_send(0)

    x_sends = []

    def send_x(i, dev, slot, u):
        c = rcopy(xs.at[own_unit(i)], xs.at[u], xss.at[slot, i], xrs.at[u], dev)
        c.start()
        x_sends.append(c)

    for i in range(q):
        if i:
            loads_x[i].wait()
        send_x(i, dev_c, 0, partner_unit(i))
        send_x(i, dev_y, 1, 2 * (i + e))
        send_x(i, dev_d, 2, 2 * (i + e) + 1)
    for i in range(1, PIECES):
        first(i)
        first_send(i)
    load_o.start()
    for c in sends_2 + loads_2:
        c.start()

    def p_copy(u):
        return rcopy(psend.at[u], precv.at[u], pss.at[u], prs.at[u], dev_x)

    def h_copy(u):
        return rcopy(h.at[0, u], h.at[1, u], hss.at[u], hrs.at[u], dev_x)

    def partial(u):
        psend[u] = dot(xs[u], w1s[...])
        p_copy(u).start()

    def stay(u):
        pown[u] = dot(xs[u], w1o[...])

    def x_wait(u):
        rcopy(xs.at[u], xs.at[u], xss.at[0, 0], xrs.at[u], dev_c).wait_recv()

    def own(u):
        i = lax.rem(u, 2)
        return jnp.logical_or(jnp.logical_and(i == 0, u < q), jnp.logical_and(i == 1, u >= 3 * q))

    def layer1(u):
        @pl.when(jnp.logical_not(own(u)))
        def _():
            x_wait(u)

        partial(u)
        stay(u)

    def activate(u):
        p_copy(u).wait_recv()
        c = (pown[u] + precv[u]).astype(BF16)
        h[0, u] = gelu(c).astype(BF16)
        h_copy(u).start()

    def z_copy(u):
        i, k = lax.rem(u, 2), u // 2
        other = jnp.logical_and(k >= e, k < e + q).astype(jnp.int32)
        late = (k >= e + q).astype(jnp.int32)
        sub = k - other * e - late * q
        swap = jnp.where(late == 1, 1 - i, i)
        dev = (cz + other - 2 * other * cz, cy, cx + swap - 2 * swap * cx)
        slot = other * (1 + swap)
        return rcopy(zp.at[u], zr.at[slot, sub], zss.at[u], zrs.at[slot, sub], dev)

    def layer2(u):
        zp[u] = dot(h[0, u], w2s[0])
        h_copy(u).wait_recv()
        zp[u] += dot(h[1, u], w2s[1])

        @pl.when(jnp.logical_not(own(u)))
        def _():
            z_copy(u).start()

    load_o.wait()
    stay(0)

    def loop(lo, hi, *stages):
        def step(u, carry):
            for stage, shift in stages:
                stage(u + shift)
            return carry

        lax.fori_loop(lo, hi, step, 0)

    loop(1, LAG + 1, (layer1, 0))
    loop(0, LAG, (activate, 0), (layer1, LAG + 1))
    for c in loads_2:
        c.wait()
    for j, b in enumerate((cy, oy)):
        rcopy(w2_ref.at[block(2 * ox + b, half)], w2s.at[j, :, block(ox, wide)], wss.at[j], wrs.at[j], dev_c).wait_recv()
    loop(LAG, n - LAG - 1, (activate, 0), (layer1, LAG + 1), (layer2, -LAG))
    loop(n - LAG - 1, n, (activate, 0), (layer2, -LAG))
    loop(n - LAG, n - 1, (layer2, 0))

    def arrived(i):
        for slot in range(3):
            rcopy(zp.at[0], zr.at[slot, i], zss.at[0], zrs.at[slot, i], dev_c).wait_recv()
        return zr[0, i] + zr[1, i] + zr[2, i]

    for i in range(q - 1):
        out_ref[pl.ds(i * G, G)] = (zp[own_unit(i)] + arrived(i)).astype(BF16)
    zp[n - 1] = dot(h[0, n - 1], w2s[0]) + arrived(q - 1)
    h_copy(n - 1).wait_recv()
    out_ref[pl.ds((q - 1) * G, G)] = (zp[n - 1] + dot(h[1, n - 1], w2s[1])).astype(BF16)

    for c in x_sends + sends_2:
        c.wait_send()

    def finish(u):
        p_copy(u).wait_send()
        h_copy(u).wait_send()

        @pl.when(jnp.logical_not(own(u)))
        def _():
            z_copy(u).wait_send()

    loop(0, n, (finish, 0))


def solution(mesh):
    def body(x, w1, w2):
        rows, depth = x.shape
        q = rows // G
        n = 4 * q
        half = w1.shape[1] // 2
        wide = w2.shape[1]
        dma = pltpu.SemaphoreType.DMA
        anywhere = pl.BlockSpec(memory_space=pl.ANY)
        return pl.pallas_call(
            kernel,
            out_shape=jax.ShapeDtypeStruct((rows, 2 * wide), BF16),
            in_specs=[anywhere] * 3,
            out_specs=pl.BlockSpec(memory_space=pltpu.VMEM),
            scratch_shapes=[
                pltpu.VMEM((n, G, depth), BF16),
                pltpu.VMEM((depth, half), BF16),
                pltpu.VMEM((depth, half), BF16),
                pltpu.VMEM((2, half, 2 * wide), BF16),
                pltpu.VMEM((n, G, half), F32),
                pltpu.VMEM((n, G, half), F32),
                pltpu.VMEM((n, G, half), F32),
                pltpu.VMEM((2, n, G, half), BF16),
                pltpu.VMEM((n, G, 2 * wide), F32),
                pltpu.VMEM((3, q, G, 2 * wide), F32),
                dma((q + PIECES + 3,)),
                dma((3, q)), dma((n,)),
                dma((2,)), dma((2,)),
                dma((n,)), dma((n,)),
                dma((n,)), dma((n,)),
                dma((n,)), dma((3, q)),
            ],
            compiler_params=pltpu.CompilerParams(
                collective_id=0, has_side_effects=True, vmem_limit_bytes=60 * 1024 * 1024,
            ),
            cost_estimate=pl.CostEstimate(flops=4 * 512 * 1024 * 2048 * 2, bytes_accessed=9 << 20, transcendentals=512 * 1024),
        )(x, w1, w2)

    return jax.shard_map(
        body,
        mesh=mesh,
        in_specs=(P(("cx", "cz"), "cy"), P("cy", ("cz", "cx")), P("cz", ("cy", "cx"))),
        out_specs=P(("cx", "cz"), "cy"),
        check_vma=False,
    )
```

```python
import functools

import jax
import jax.numpy as jnp
from jax import lax
from jax.experimental import pallas as pl
from jax.experimental.pallas import tpu as pltpu
from jax.sharding import PartitionSpec as P

MESH = pl.DeviceIdType.MESH
F32 = jnp.float32
BF16 = jnp.bfloat16
G = 64
LAG = 1
STARTS = (0, 128, 512, 1024)
LAST = 4


def gelu(c):
    c = c.astype(F32)
    return 0.5 * c * (1.0 + jnp.tanh(0.7978845608028654 * (c + 0.044715 * (c * c * c))))


def dot(a, b):
    return jnp.dot(a, b, preferred_element_type=F32)


def kernel(x_ref, w1_ref, w2_ref, out_ref,
           xs, w1s, w1o, w2s, psend, precv, pown, h, zp, zr,
           lsem, xss, xrs, wss, wrs, pss, prs, hss, hrs, lss, lrs, zss, zrs):
    cz, cy, cx = (lax.axis_index(a) for a in ("cz", "cy", "cx"))
    oz, oy, ox = 1 - cz, 1 - cy, 1 - cx
    dev_x = (cz, oy, cx)
    dev_c = (cz, cy, ox)
    dev_y = (oz, cy, cx)
    dev_d = (oz, cy, ox)

    rows = x_ref.shape[0]
    q = rows // G
    n = 4 * q
    e = q // 2
    half = w1_ref.shape[1] // 2
    wide = w2_ref.shape[1]
    pieces = [pl.ds(a, b - a) for a, b in zip(STARTS, STARTS[1:])]
    count = len(pieces)
    last = [pl.ds(k * (half // LAST), half // LAST) for k in range(LAST)]

    def own_unit(i):
        return 2 * i if i < e else 2 * (i + q) + 1

    def partner_unit(i):
        return 2 * i + 1 if i < e else 2 * (i + q)

    def rcopy(src, dst, ss, rs, dev):
        return pltpu.make_async_remote_copy(src_ref=src, dst_ref=dst, send_sem=ss, recv_sem=rs, device_id=dev,
                                            device_id_type=MESH)

    def block(i, size):
        return pl.ds(pl.multiple_of(i * size, size), size)

    loads_x = [pltpu.make_async_copy(x_ref.at[pl.ds(i * G, G)], xs.at[own_unit(i)], lsem.at[i]) for i in range(q)]
    loads_s = [pltpu.make_async_copy(w1_ref.at[:, pl.ds(pl.multiple_of(oy * half + c.start, 128), c.size)], w1s.at[:, c],
                                     lsem.at[q + i]) for i, c in enumerate(pieces)]
    load_o = pltpu.make_async_copy(w1_ref.at[:, block(cy, half)], w1o, lsem.at[q + count])
    loads_2 = [pltpu.make_async_copy(w2_ref.at[block(2 * cx + b, half)], w2s.at[j, :, block(cx, wide)],
                                     lsem.at[q + count + 1 + j]) for j, b in enumerate((cy, oy))]
    sends_2 = [rcopy(w2_ref.at[block(2 * ox + b, half)], w2s.at[j, :, block(cx, wide)], wss.at[j], wrs.at[j], dev_c)
               for j, b in enumerate((cy, oy))]
    for c in loads_x[:1] + loads_s[:1] + loads_x[1:] + loads_s[1:]:
        c.start()

    barrier = pltpu.get_barrier_semaphore()
    for dev in (dev_x, dev_c, dev_y, dev_d):
        pl.semaphore_signal(barrier, inc=1, device_id=dev, device_id_type=MESH)

    def first(i):
        cols = pieces[i]
        loads_s[i].wait()
        psend[0, :, cols] = dot(xs[0], w1s[:, cols])

    def first_send(i):
        cols = pieces[i]
        rcopy(psend.at[0, :, cols], precv.at[0, :, cols], pss.at[0], prs.at[0], dev_x).start()

    loads_x[0].wait()
    first(0)
    pl.semaphore_wait(barrier, 4)
    first_send(0)

    x_sends = []

    def send_x(i, dev, slot, u):
        c = rcopy(xs.at[own_unit(i)], xs.at[u], xss.at[slot, i], xrs.at[u], dev)
        c.start()
        x_sends.append(c)

    for i in range(q):
        if i:
            loads_x[i].wait()
        send_x(i, dev_c, 0, partner_unit(i))
        send_x(i, dev_y, 1, 2 * (i + e))
        send_x(i, dev_d, 2, 2 * (i + e) + 1)
    for i in range(1, count):
        first(i)
        first_send(i)
    load_o.start()
    for c in sends_2 + loads_2:
        c.start()

    def p_copy(u):
        return rcopy(psend.at[u], precv.at[u], pss.at[u], prs.at[u], dev_x)

    def h_copy(u):
        return rcopy(h.at[0, u], h.at[1, u], hss.at[u], hrs.at[u], dev_x)

    def partial(u):
        psend[u] = dot(xs[u], w1s[...])
        p_copy(u).start()

    def stay(u):
        pown[u] = dot(xs[u], w1o[...])

    def x_wait(u):
        rcopy(xs.at[u], xs.at[u], xss.at[0, 0], xrs.at[u], dev_c).wait_recv()

    def own(u):
        i = lax.rem(u, 2)
        return jnp.logical_or(jnp.logical_and(i == 0, u < q), jnp.logical_and(i == 1, u >= 3 * q))

    def layer1(u):
        @pl.when(jnp.logical_not(own(u)))
        def _():
            x_wait(u)

        partial(u)
        stay(u)

    def activate(u):
        p_copy(u).wait_recv()
        c = (pown[u] + precv[u]).astype(BF16)
        h[0, u] = gelu(c).astype(BF16)
        h_copy(u).start()

    def h_piece(k):
        return rcopy(h.at[0, n - 1, :, last[k]], h.at[1, n - 1, :, last[k]], lss.at[k], lrs.at[k], dev_x)

    def activate_last():
        p_copy(n - 1).wait_recv()
        for k in range(LAST):
            c = (pown[n - 1, :, last[k]] + precv[n - 1, :, last[k]]).astype(BF16)
            h[0, n - 1, :, last[k]] = gelu(c).astype(BF16)
            h_piece(k).start()

    def z_copy(u):
        i, k = lax.rem(u, 2), u // 2
        other = jnp.logical_and(k >= e, k < e + q).astype(jnp.int32)
        late = (k >= e + q).astype(jnp.int32)
        sub = k - other * e - late * q
        swap = jnp.where(late == 1, 1 - i, i)
        dev = (cz + other - 2 * other * cz, cy, cx + swap - 2 * swap * cx)
        slot = other * (1 + swap)
        return rcopy(zp.at[u], zr.at[slot, sub], zss.at[u], zrs.at[slot, sub], dev)

    def layer2(u):
        zp[u] = dot(h[0, u], w2s[0])
        h_copy(u).wait_recv()
        zp[u] += dot(h[1, u], w2s[1])

        @pl.when(jnp.logical_not(own(u)))
        def _():
            z_copy(u).start()

    load_o.wait()
    stay(0)

    def loop(lo, hi, *stages):
        def step(u, carry):
            for stage, shift in stages:
                stage(u + shift)
            return carry

        lax.fori_loop(lo, hi, step, 0)

    loop(1, LAG + 1, (layer1, 0))
    loop(0, LAG, (activate, 0), (layer1, LAG + 1))
    for c in loads_2:
        c.wait()
    for j, b in enumerate((cy, oy)):
        rcopy(w2_ref.at[block(2 * ox + b, half)], w2s.at[j, :, block(ox, wide)], wss.at[j], wrs.at[j], dev_c).wait_recv()
    loop(LAG, n - LAG - 1, (activate, 0), (layer1, LAG + 1), (layer2, -LAG))
    loop(n - LAG - 1, n - 1, (activate, 0), (layer2, -LAG))
    activate_last()
    loop(n - 1 - LAG, n - 1, (layer2, 0))

    def arrived(i):
        for slot in range(3):
            rcopy(zp.at[0], zr.at[slot, i], zss.at[0], zrs.at[slot, i], dev_c).wait_recv()
        return zr[0, i] + zr[1, i] + zr[2, i]

    for i in range(q - 1):
        out_ref[pl.ds(i * G, G)] = (zp[own_unit(i)] + arrived(i)).astype(BF16)
    zp[n - 1] = dot(h[0, n - 1], w2s[0]) + arrived(q - 1)

    for c in x_sends + sends_2:
        c.wait_send()

    def finish(u):
        p_copy(u).wait_send()

        @pl.when(u < n - 1)
        def _():
            h_copy(u).wait_send()

        @pl.when(jnp.logical_not(own(u)))
        def _():
            z_copy(u).wait_send()

    loop(0, n, (finish, 0))
    for k in range(LAST - 1):
        h_piece(k).wait_recv()
        zp[n - 1] += dot(h[1, n - 1, :, last[k]], w2s[1, last[k]])
    h_piece(LAST - 1).wait_recv()
    z = zp[n - 1] + dot(h[1, n - 1, :, last[LAST - 1]], w2s[1, last[LAST - 1]])
    out_ref[pl.ds((q - 1) * G, G)] = z.astype(BF16)
    for k in range(LAST):
        h_piece(k).wait_send()


def solution(mesh):
    def body(x, w1, w2):
        rows, depth = x.shape
        q = rows // G
        n = 4 * q
        half = w1.shape[1] // 2
        wide = w2.shape[1]
        dma = pltpu.SemaphoreType.DMA
        anywhere = pl.BlockSpec(memory_space=pl.ANY)
        return pl.pallas_call(
            kernel,
            out_shape=jax.ShapeDtypeStruct((rows, 2 * wide), BF16),
            in_specs=[anywhere] * 3,
            out_specs=pl.BlockSpec(memory_space=pltpu.VMEM),
            scratch_shapes=[
                pltpu.VMEM((n, G, depth), BF16),
                pltpu.VMEM((depth, half), BF16),
                pltpu.VMEM((depth, half), BF16),
                pltpu.VMEM((2, half, 2 * wide), BF16),
                pltpu.VMEM((n, G, half), F32),
                pltpu.VMEM((n, G, half), F32),
                pltpu.VMEM((n, G, half), F32),
                pltpu.VMEM((2, n, G, half), BF16),
                pltpu.VMEM((n, G, 2 * wide), F32),
                pltpu.VMEM((3, q, G, 2 * wide), F32),
                dma((q + len(STARTS) + 2,)),
                dma((3, q)), dma((n,)),
                dma((2,)), dma((2,)),
                dma((n,)), dma((n,)),
                dma((n,)), dma((n,)),
                dma((LAST,)), dma((LAST,)),
                dma((n,)), dma((3, q)),
            ],
            compiler_params=pltpu.CompilerParams(
                collective_id=0, has_side_effects=True, vmem_limit_bytes=54784 * 1024,
            ),
            cost_estimate=pl.CostEstimate(flops=4 * 512 * 1024 * 2048 * 2, bytes_accessed=9 << 20, transcendentals=512 * 1024),
        )(x, w1, w2)

    return jax.shard_map(
        body,
        mesh=mesh,
        in_specs=(P(("cx", "cz"), "cy"), P("cy", ("cz", "cx")), P("cz", ("cy", "cx"))),
        out_specs=P(("cx", "cz"), "cy"),
        check_vma=False,
    )
```

```python
import functools

import jax
import jax.numpy as jnp
from jax import lax
from jax.experimental import pallas as pl
from jax.experimental.pallas import tpu as pltpu
from jax.sharding import PartitionSpec as P

MESH = pl.DeviceIdType.MESH
F32 = jnp.float32
BF16 = jnp.bfloat16
G = 64
LAG = 1
STARTS = (0, 256, 512, 1024)
LAST = 4


def gelu(c):
    c = c.astype(F32)
    return 0.5 * c * (1.0 + jnp.tanh(0.7978845608028654 * (c + 0.044715 * (c * c * c))))


def dot(a, b):
    return jnp.dot(a, b, preferred_element_type=F32)


def kernel(x_ref, w1_ref, w2_ref, out_ref,
           xs, w1s, w1o, w2s, psend, precv, pown, h, zp, zr,
           entered, lsem, xss, xrs, wss, wrs, pss, prs, hss, hrs, lrs, zss, zrs):
    cz, cy, cx = (lax.axis_index(a) for a in ("cz", "cy", "cx"))
    oz, oy, ox = 1 - cz, 1 - cy, 1 - cx
    dev_x = (cz, oy, cx)
    dev_c = (cz, cy, ox)
    dev_y = (oz, cy, cx)
    dev_d = (oz, cy, ox)

    rows = x_ref.shape[0]
    q = rows // G
    n = 4 * q
    e = q // 2
    half = w1_ref.shape[1] // 2
    wide = w2_ref.shape[1]
    pieces = [pl.ds(a, b - a) for a, b in zip(STARTS, STARTS[1:])]
    count = len(pieces)
    last = [pl.ds(k * (half // LAST), half // LAST) for k in range(LAST)]

    def own_unit(i):
        return 2 * i if i < e else 2 * (i + q) + 1

    def partner_unit(i):
        return 2 * i + 1 if i < e else 2 * (i + q)

    def rcopy(src, dst, ss, rs, dev):
        return pltpu.make_async_remote_copy(src_ref=src, dst_ref=dst, send_sem=ss, recv_sem=rs, device_id=dev,
                                            device_id_type=MESH)

    def block(i, size):
        return pl.ds(pl.multiple_of(i * size, size), size)

    loads_x = [pltpu.make_async_copy(x_ref.at[pl.ds(i * G, G)], xs.at[own_unit(i)], lsem.at[i]) for i in range(q)]
    loads_s = [pltpu.make_async_copy(w1_ref.at[:, pl.ds(pl.multiple_of(oy * half + c.start, 128), c.size)], w1s.at[:, c],
                                     lsem.at[q + i]) for i, c in enumerate(pieces)]
    load_o = pltpu.make_async_copy(w1_ref.at[:, block(cy, half)], w1o, lsem.at[q + count])
    loads_2 = [pltpu.make_async_copy(w2_ref.at[block(2 * cx + b, half)], w2s.at[j, :, block(cx, wide)],
                                     lsem.at[q + count + 1]) for j, b in enumerate((cy, oy))]
    sends_2 = [rcopy(w2_ref.at[block(2 * ox + b, half)], w2s.at[j, :, block(cx, wide)], wss, wrs, dev_c)
               for j, b in enumerate((cy, oy))]
    for c in loads_x[:1] + loads_s[:1] + loads_x[1:] + loads_s[1:]:
        c.start()

    barrier = pltpu.get_barrier_semaphore()

    def signal(sem, *devs):
        for dev in devs:
            pl.semaphore_signal(sem, inc=1, device_id=dev, device_id_type=MESH)

    signal(barrier, dev_x, dev_c)

    @pl.when(cz == 0)
    def _():
        signal(barrier, dev_y, dev_d)

    def first(i):
        cols = pieces[i]
        loads_s[i].wait()
        psend[0, :, cols] = dot(xs[0], w1s[:, cols])

    def first_send(i):
        cols = pieces[i]
        rcopy(psend.at[0, :, cols], precv.at[0, :, cols], pss, prs.at[0], dev_x).start()

    def p_copy(u):
        return rcopy(psend.at[u], precv.at[u], pss, prs.at[u], dev_x)

    def h_copy(u):
        return rcopy(h.at[0, u], h.at[1, u], hss, hrs.at[u], dev_x)

    loads_x[0].wait()
    first(0)
    pl.semaphore_wait(barrier, 2 + 2 * cz)

    @pl.when(cz == 1)
    def _():
        signal(entered, dev_y, dev_d)

    @pl.when(cx == 0)
    def _():
        first_send(0)

    def send_x(i, dev, u):
        rcopy(xs.at[own_unit(i)], xs.at[u], xss, xrs.at[u], dev).start()

    for i in range(q):
        if i:
            loads_x[i].wait()
        send_x(i, dev_c, partner_unit(i))
    for i in range(1, count):
        first(i)

        @pl.when(cx == 0)
        def _():
            first_send(i)

    @pl.when(cx == 1)
    def _():
        p_copy(0).start()

    @pl.when(cz == 0)
    def _():
        pl.semaphore_wait(entered, 2)

    for i in range(q):
        send_x(i, dev_y, 2 * (i + e))
        send_x(i, dev_d, 2 * (i + e) + 1)
    load_o.start()
    for c in sends_2 + loads_2:
        c.start()

    def partial(u):
        psend[u] = dot(xs[u], w1s[...])
        p_copy(u).start()

    def stay(u):
        pown[u] = dot(xs[u], w1o[...])

    def x_wait(u):
        rcopy(xs.at[u], xs.at[u], xss, xrs.at[u], dev_c).wait_recv()

    def own(u):
        i = lax.rem(u, 2)
        return jnp.logical_or(jnp.logical_and(i == 0, u < q), jnp.logical_and(i == 1, u >= 3 * q))

    def layer1(u):
        @pl.when(jnp.logical_not(own(u)))
        def _():
            x_wait(u)

        partial(u)
        stay(u)

    def activate(u):
        p_copy(u).wait_recv()
        c = (pown[u] + precv[u]).astype(BF16)
        h[0, u] = gelu(c).astype(BF16)
        h_copy(u).start()

    def h_piece(k):
        return rcopy(h.at[0, n - 1, :, last[k]], h.at[1, n - 1, :, last[k]], hss, lrs.at[k], dev_x)

    def activate_last():
        p_copy(n - 1).wait_recv()
        for k in range(LAST):
            c = (pown[n - 1, :, last[k]] + precv[n - 1, :, last[k]]).astype(BF16)
            h[0, n - 1, :, last[k]] = gelu(c).astype(BF16)
            h_piece(k).start()

    def z_copy(u):
        i, k = lax.rem(u, 2), u // 2
        other = jnp.logical_and(k >= e, k < e + q).astype(jnp.int32)
        late = (k >= e + q).astype(jnp.int32)
        sub = k - other * e - late * q
        swap = jnp.where(late == 1, 1 - i, i)
        dev = (cz + other - 2 * other * cz, cy, cx + swap - 2 * swap * cx)
        slot = other * (1 + swap)
        return rcopy(zp.at[u], zr.at[sub, slot], zss, zrs.at[sub], dev)

    def layer2(u):
        zp[u] = dot(h[0, u], w2s[0])
        h_copy(u).wait_recv()
        zp[u] += dot(h[1, u], w2s[1])

        @pl.when(jnp.logical_not(own(u)))
        def _():
            z_copy(u).start()

    load_o.wait()
    stay(0)

    def loop(lo, hi, *stages):
        def step(u, carry):
            for stage, shift in stages:
                stage(u + shift)
            return carry

        lax.fori_loop(lo, hi, step, 0)

    loop(1, LAG + 1, (layer1, 0))
    loop(0, LAG, (activate, 0), (layer1, LAG + 1))
    theirs = w2s.at[:, :, block(ox, wide)]
    mine = w2s.at[:, :, block(cx, wide)]
    pltpu.make_async_copy(mine, mine, lsem.at[q + count + 1]).wait()
    rcopy(theirs, theirs, wss, wrs, dev_c).wait_recv()
    loop(LAG, n - LAG - 1, (activate, 0), (layer1, LAG + 1), (layer2, -LAG))
    loop(n - LAG - 1, n - 1, (activate, 0), (layer2, -LAG))
    activate_last()
    loop(n - 1 - LAG, n - 1, (layer2, 0))

    def arrived(i):
        rcopy(zr.at[i], zr.at[i], zss, zrs.at[i], dev_c).wait_recv()
        return zr[i, 0] + zr[i, 1] + zr[i, 2]

    for i in range(q - 1):
        out_ref[pl.ds(i * G, G)] = (zp[own_unit(i)] + arrived(i)).astype(BF16)
    zp[n - 1] = dot(h[0, n - 1], w2s[0])

    def sent(ref, sem):
        rcopy(ref, ref, sem, xrs.at[0], dev_x).wait_send()

    sent(xs.at[pl.ds(0, 3 * q)], xss)
    sent(theirs, wss)
    sent(psend, pss)
    sent(zp.at[pl.ds(0, n - q)], zss)
    for k in range(LAST - 1):
        h_piece(k).wait_recv()
        zp[n - 1] += dot(h[1, n - 1, :, last[k]], w2s[1, last[k]])
    zp[n - 1] += arrived(q - 1)
    h_piece(LAST - 1).wait_recv()
    z = zp[n - 1] + dot(h[1, n - 1, :, last[LAST - 1]], w2s[1, last[LAST - 1]])
    out_ref[pl.ds((q - 1) * G, G)] = z.astype(BF16)
    sent(h.at[0], hss)


def solution(mesh):
    def body(x, w1, w2):
        rows, depth = x.shape
        q = rows // G
        n = 4 * q
        half = w1.shape[1] // 2
        wide = w2.shape[1]
        dma = pltpu.SemaphoreType.DMA
        anywhere = pl.BlockSpec(memory_space=pl.ANY)
        return pl.pallas_call(
            kernel,
            out_shape=jax.ShapeDtypeStruct((rows, 2 * wide), BF16),
            in_specs=[anywhere] * 3,
            out_specs=pl.BlockSpec(memory_space=pltpu.VMEM),
            scratch_shapes=[
                pltpu.VMEM((n, G, depth), BF16),
                pltpu.VMEM((depth, half), BF16),
                pltpu.VMEM((depth, half), BF16),
                pltpu.VMEM((2, half, 2 * wide), BF16),
                pltpu.VMEM((n, G, half), F32),
                pltpu.VMEM((n, G, half), F32),
                pltpu.VMEM((n, G, half), F32),
                pltpu.VMEM((2, n, G, half), BF16),
                pltpu.VMEM((n, G, 2 * wide), F32),
                pltpu.VMEM((q, 3, G, 2 * wide), F32),
                pltpu.SemaphoreType.REGULAR,
                dma((q + len(STARTS) + 1,)),
                dma, dma((n,)),
                dma, dma,
                dma, dma((n,)),
                dma, dma((n,)), dma((LAST,)),
                dma, dma((q,)),
            ],
            compiler_params=pltpu.CompilerParams(
                collective_id=0, has_side_effects=True, vmem_limit_bytes=54784 * 1024,
            ),
            cost_estimate=pl.CostEstimate(flops=4 * 512 * 1024 * 2048 * 2, bytes_accessed=9 << 20, transcendentals=512 * 1024),
        )(x, w1, w2)

    return jax.shard_map(
        body,
        mesh=mesh,
        in_specs=(P(("cx", "cz"), "cy"), P("cy", ("cz", "cx")), P("cz", ("cy", "cx"))),
        out_specs=P(("cx", "cz"), "cy"),
        check_vma=False,
    )
```

```python
import jax
import jax.numpy as jnp
from jax import lax
from jax.experimental import pallas as pl
from jax.experimental.pallas import tpu as pltpu
from jax.sharding import PartitionSpec as P

MESH = pl.DeviceIdType.MESH
F32 = jnp.float32
BF16 = jnp.bfloat16
G = 64
FIRST = (0, 128, 512, 1024)
LAST = (0, 512, 768, 1024)
S, R = 4, 32


def gelu(c):
    c = c.astype(F32)
    return 0.5 * c * (1.0 + jnp.tanh(0.7978845608028654 * (c + 0.044715 * (c * c * c))))


def hidden(a, b):
    return gelu((a + b).astype(BF16)).astype(BF16)


def dot(a, b):
    return jnp.dot(a, b, preferred_element_type=F32)


def spans(edges):
    return [pl.ds(a, b - a) for a, b in zip(edges, edges[1:])]


def kernel(x_ref, w1_ref, w2_ref, out_ref,
           xs, w1s, w1o, w2s, psend, precv, pown, pextra, h, zp, zr,
           entered, lsem, sent, hsent, xrs, wrs, prs, hrs, lrs, ers, zrs):
    cz, cy, cx = (lax.axis_index(a) for a in ("cz", "cy", "cx"))
    oz, oy, ox = 1 - cz, 1 - cy, 1 - cx
    dev_x = (cz, oy, cx)
    dev_c = (cz, cy, ox)
    dev_y = (oz, cy, cx)
    dev_d = (oz, cy, ox)

    rows = x_ref.shape[0]
    q = rows // G
    n = 4 * q
    e = q // 2
    half = w1_ref.shape[1] // 2
    wide = w2_ref.shape[1]
    first_cols, last_cols = spans(FIRST), spans(LAST)
    count = len(first_cols)

    def own_unit(i):
        return 2 * i if i < e else 2 * (i + q) + 1

    def partner_unit(i):
        return 2 * i + 1 if i < e else 2 * (i + q)

    def own(u):
        i = lax.rem(u, 2)
        return jnp.logical_or(jnp.logical_and(i == 0, u < q), jnp.logical_and(i == 1, u >= 3 * q))

    def rcopy(src, dst, ss, rs, dev):
        return pltpu.make_async_remote_copy(src_ref=src, dst_ref=dst, send_sem=ss, recv_sem=rs, device_id=dev,
                                            device_id_type=MESH)

    def block(i, size):
        return pl.ds(pl.multiple_of(i * size, size), size)

    def when(*conditions):
        c = conditions[0]
        for d in conditions[1:]:
            c = jnp.logical_and(c, d)
        return pl.when(c)

    loads_x = [pltpu.make_async_copy(x_ref.at[pl.ds(i * G, G)], xs.at[own_unit(i)], lsem.at[i]) for i in range(q)]
    loads_1 = [pltpu.make_async_copy(w1_ref.at[:, pl.ds(pl.multiple_of(oy * half + c.start, 128), c.size)], w1s.at[:, c],
                                     lsem.at[q + i]) for i, c in enumerate(first_cols)]
    load_o = pltpu.make_async_copy(w1_ref.at[:, block(cy, half)], w1o, lsem.at[0])
    mine = w2s.at[:, :, block(cx, wide)]
    theirs = w2s.at[:, :, block(ox, wide)]
    loads_2 = [pltpu.make_async_copy(w2_ref.at[block(2 * cx + b, half)], mine.at[j], lsem.at[q])
               for j, b in enumerate((cy, oy))]
    sends_2 = [rcopy(w2_ref.at[block(2 * ox + b, half)], mine.at[j], sent, wrs, dev_c) for j, b in enumerate((cy, oy))]
    for c in loads_1[:1] + loads_x[:1] + loads_1[1:] + loads_x[1:]:
        c.start()

    barrier = pltpu.get_barrier_semaphore()

    def signal(sem, *devs):
        for dev in devs:
            pl.semaphore_signal(sem, inc=1, device_id=dev, device_id_type=MESH)

    signal(barrier, dev_x, dev_c)

    @pl.when(cz == 0)
    def _():
        signal(barrier, dev_y, dev_d)

    def p_copy(u, r=slice(None)):
        return rcopy(psend.at[u, r], precv.at[u, r], sent, prs.at[u], dev_x)

    def h_copy(u, r=slice(None)):
        return rcopy(h.at[0, u, r], h.at[1, u, r], hsent, hrs.at[u], dev_x)

    def h_piece(c):
        return rcopy(h.at[0, n - 1, :, last_cols[c]], h.at[1, n - 1, :, last_cols[c]], hsent, lrs.at[c], dev_x)

    top, rest = pl.ds(0, R), pl.ds(R, G - R)

    def extra_p():
        return rcopy(pown.at[S, top], pextra, sent, ers, dev_x)

    def extra_h():
        return rcopy(h.at[1, S, top], h.at[0, S, top], hsent, ers, dev_x)

    def first(i):
        c = first_cols[i]
        loads_1[i].wait()
        psend[0, :, c] = dot(xs[0], w1s[:, c])

    def first_send(i):
        c = first_cols[i]
        rcopy(psend.at[0, :, c], precv.at[0, :, c], sent, prs.at[0], dev_x).start()

    loads_x[0].wait()
    first(0)
    pl.semaphore_wait(barrier, 2 + 2 * cz)
    first_send(0)

    @pl.when(cz == 1)
    def _():
        signal(entered, dev_y, dev_d)

    def send_x(i, dev, u):
        rcopy(xs.at[own_unit(i)], xs.at[u], sent, xrs.at[u // 2], dev).start()

    for i in range(q):
        if i:
            loads_x[i].wait()
        send_x(i, dev_c, partner_unit(i))
    for i in range(1, count):
        first(i)
        first_send(i)

    @pl.when(cz == 0)
    def _():
        pl.semaphore_wait(entered, 2)

    for i in range(q):
        send_x(i, dev_y, 2 * (i + e))
        send_x(i, dev_d, 2 * (i + e) + 1)
    load_o.start()
    for c in sends_2 + loads_2:
        c.start()

    def partial(u):
        psend[u] = dot(xs[u], w1s[...])

        @when(jnp.logical_or(u != S, cy == 0))
        def _():
            p_copy(u).start()

        @when(u == S, cy == 1)
        def _():
            p_copy(S, rest).start()

    def stay(u):
        pown[u] = dot(xs[u], w1o[...])

        @when(u == S, cy == 0)
        def _():
            extra_p().start()

    def x_wait(u):
        k = u // 2
        inner = jnp.logical_and(u >= q, u < 3 * q)

        @when(inner, lax.rem(u, 2) == 0)
        def _():
            two = xs.at[pl.ds(u, 2)]
            rcopy(two, two, sent, xrs.at[k], dev_c).wait_recv()

        @when(jnp.logical_not(inner), jnp.logical_not(own(u)))
        def _():
            rcopy(xs.at[u], xs.at[u], sent, xrs.at[k], dev_c).wait_recv()

    def layer1(u):
        x_wait(u)
        partial(u)
        stay(u)

    def activate(u):
        @when(jnp.logical_or(u != S, cy == 1))
        def _():
            p_copy(u).wait_recv()
            h[0, u] = hidden(pown[u], precv[u])

            @pl.when(u > 0)
            def _():
                h_copy(u).start()

        @when(u == S, cy == 0)
        def _():
            p_copy(S, rest).wait_recv()
            h[0, S, rest] = hidden(pown[S, rest], precv[S, rest])
            h_copy(S, rest).start()

        @when(u == S, cy == 1)
        def _():
            extra_p().wait_recv()
            h[1, S, top] = hidden(psend[S, top], pextra[...])
            extra_h().start()

    def activate_last():
        p_copy(n - 1).wait_recv()
        for k, c in enumerate(last_cols):
            h[0, n - 1, :, c] = hidden(pown[n - 1, :, c], precv[n - 1, :, c])
            h_piece(k).start()

    def z_copy(u):
        i, k = lax.rem(u, 2), u // 2
        other = jnp.logical_and(k >= e, k < e + q).astype(jnp.int32)
        late = (k >= e + q).astype(jnp.int32)
        sub = k - other * e - late * q
        swap = jnp.where(late == 1, 1 - i, i)
        dev = (cz + other - 2 * other * cz, cy, cx + swap - 2 * swap * cx)
        slot = other * (1 + swap)
        return rcopy(zp.at[u], zr.at[sub, slot], sent, zrs.at[sub], dev)

    def layer2(u):
        @when(u == S, cy == 0)
        def _():
            extra_h().wait_recv()

        zp[u] = dot(h[0, u], w2s[0])

        @when(jnp.logical_or(u != S, cy == 0))
        def _():
            h_copy(u).wait_recv()

        @when(u == S, cy == 1)
        def _():
            h_copy(S, rest).wait_recv()

        zp[u] += dot(h[1, u], w2s[1])

        @when(jnp.logical_not(own(u)))
        def _():
            z_copy(u).start()

    load_o.wait()
    stay(0)

    def loop(lo, hi, *stages):
        def step(u, carry):
            for stage, shift in stages:
                stage(u + shift)
            return carry

        lax.fori_loop(lo, hi, step, 0)

    loop(1, 2, (layer1, 0))
    loop(0, 2, (activate, 0), (layer1, 2))
    pltpu.make_async_copy(mine, mine, lsem.at[q]).wait()
    rcopy(theirs, theirs, sent, wrs, dev_c).wait_recv()
    loop(2, n - 2, (activate, 0), (layer1, 2), (layer2, -1))
    h_copy(0).start()
    loop(n - 2, n - 1, (activate, 0), (layer2, -1))
    activate_last()
    for u in (n - 1, n - 2):
        zp[u] = dot(h[0, u], w2s[0])
    loop(0, 1, (layer2, 0))

    def arrived(i):
        rcopy(zr.at[i], zr.at[i], sent, zrs.at[i], dev_c).wait_recv()
        return zr[i, 0] + zr[i, 1] + zr[i, 2]

    for i in range(q - 1):
        out_ref[pl.ds(i * G, G)] = (zp[own_unit(i)] + arrived(i)).astype(BF16)
    h_copy(n - 2).wait_recv()
    zp[n - 2] += dot(h[1, n - 2], w2s[1])
    z_copy(jnp.int32(n - 2)).start()

    def left(sem, *refs):
        for ref in refs:
            rcopy(ref, ref, sem, ers, dev_x).wait_send()

    left(sent, xs.at[pl.ds(0, 3 * q)], theirs, psend.at[pl.ds(1, n - 1)], zp.at[pl.ds(0, n - q)])

    @pl.when(cy == 0)
    def _():
        left(sent, psend.at[S], pown.at[S, top])

    @pl.when(cy == 1)
    def _():
        left(sent, psend.at[S, rest])

    for k, c in enumerate(last_cols):
        if k == len(last_cols) - 1:
            zp[n - 1] += arrived(q - 1)
        h_piece(k).wait_recv()
        z = zp[n - 1] + dot(h[1, n - 1, :, c], w2s[1, c])
        if k < len(last_cols) - 1:
            zp[n - 1] = z
    out_ref[pl.ds((q - 1) * G, G)] = z.astype(BF16)

    left(hsent, h.at[0, pl.ds(0, n - 1)])

    @pl.when(cy == 0)
    def _():
        left(hsent, h.at[0, S, rest])

    @pl.when(cy == 1)
    def _():
        left(hsent, h.at[0, S], h.at[1, S, top])


def solution(mesh):
    def body(x, w1, w2):
        rows, depth = x.shape
        q = rows // G
        n = 4 * q
        half = w1.shape[1] // 2
        wide = w2.shape[1]
        dma = pltpu.SemaphoreType.DMA
        anywhere = pl.BlockSpec(memory_space=pl.ANY)
        return pl.pallas_call(
            kernel,
            out_shape=jax.ShapeDtypeStruct((rows, 2 * wide), BF16),
            in_specs=[anywhere] * 3,
            out_specs=pl.BlockSpec(memory_space=pltpu.VMEM),
            scratch_shapes=[
                pltpu.VMEM((n, G, depth), BF16),
                pltpu.VMEM((depth, half), BF16),
                pltpu.VMEM((depth, half), BF16),
                pltpu.VMEM((2, half, 2 * wide), BF16),
                pltpu.VMEM((n, G, half), F32),
                pltpu.VMEM((n, G, half), F32),
                pltpu.VMEM((n, G, half), F32),
                pltpu.VMEM((R, half), F32),
                pltpu.VMEM((2, n, G, half), BF16),
                pltpu.VMEM((n, G, 2 * wide), F32),
                pltpu.VMEM((q, 3, G, 2 * wide), F32),
                pltpu.SemaphoreType.REGULAR,
                dma((q + len(FIRST) - 1,)),
                dma, dma,
                dma((n // 2,)), dma, dma((n,)), dma((n - 1,)), dma((len(LAST) - 1,)), dma, dma((q,)),
            ],
            compiler_params=pltpu.CompilerParams(
                collective_id=0, has_side_effects=True, vmem_limit_bytes=54784 * 1024,
            ),
            cost_estimate=pl.CostEstimate(flops=4 * 512 * 1024 * 2048 * 2, bytes_accessed=9 << 20, transcendentals=512 * 1024),
        )(x, w1, w2)

    return jax.shard_map(
        body,
        mesh=mesh,
        in_specs=(P(("cx", "cz"), "cy"), P("cy", ("cz", "cx")), P("cz", ("cy", "cx"))),
        out_specs=P(("cx", "cz"), "cy"),
        check_vma=False,
    )
```
